32 devices in a mesh: samp: 8 (over y, x, core), snp: 4 (over z).
Axes of the slice: x: 2, y: 2, z: 4, core: 2. Of those that a mesh axis runs over, the one named last changes fastest.
Arguments:
- genotypes: bfloat16 [8192, 16384], P('samp', 'snp'), may hold values from -6 to 6
- probes: bfloat16 [8, 8192], P(None, 'samp'), may hold values from -6 to 6
- env_label: int32 [8192], P('samp'), may hold values from 0 to 7
- variances: float32 [3], replicated, may hold values from 0.25 to 1
Outputs:
- first: float32 [8, 8192], P(None, 'samp')
- second: float32 [8, 8192], P(None, 'samp')
The draws below stay inside these ranges and needn't reach their ends.
All inputs are finite; a program needn't handle non-finite values.
Results may differ from the reference program's by a relative error of at most 0.0018.
Values may be sent and summed in bfloat16 or wider, within the bound.
No kernel may reach another device: no remote copies, remote signals or barrier semaphores. Data moves between devices by JAX's collectives and lax.ppermute only.
A program may use at most 64 MiB of HBM per device.

```python
import math
import jax
import jax.numpy as jnp
from jax import lax

SNPS = 16384
PROBES = 8
ENVS = 8
SAMPLES = 8192


def place_ends(drawn, key, low, largest):
    place = [jax.random.randint(jax.random.fold_in(key, axis), (), 0, length) for axis, length in enumerate(drawn.shape)]
    widest = drawn.shape.index(max(drawn.shape))
    neighbour = place[:widest] + [(place[widest] + 1) % drawn.shape[widest]] + place[widest + 1:]
    return drawn.at[tuple(place)].set(low).at[tuple(neighbour)].set(largest)


def block_scale(stream_key, shape, cuts, low, largest):
    def one(dim, shards_of):
        draws = jax.random.uniform(jax.random.fold_in(jax.random.fold_in(stream_key, 6), dim), (shards_of,), jnp.float32, low / len(cuts), largest / len(cuts))
        return jnp.repeat(jnp.exp(draws), shape[dim] // shards_of).reshape((-1,) + (1,) * (len(shape) - dim - 1))

    factor_of = one(*cuts[0])
    for cut in cuts[1:]:
        factor_of = factor_of * one(*cut)
    return factor_of


def centred(key, shape, spread, bound, split=(), kind=jnp.bfloat16):
    gain = block_scale(key, shape, split, -0.22, 0.18) if split else 1.0
    result = jax.random.normal(key, shape, jnp.float32) * spread * gain
    return jnp.minimum(jnp.maximum(result, -bound), bound).astype(kind)


def setup_inputs(seed: int = 0) -> dict:
    streams_of = jax.random.split(jax.random.key(seed), 5)
    return {
        "genotypes": centred(streams_of[0], (SAMPLES, SNPS), 1.0, 6.0, ((0, 8), (1, 4))),
        "probes": centred(streams_of[1], (PROBES, SAMPLES), 1.0, 6.0, ((1, 8),)),
        "env_label": place_ends(jax.random.randint(streams_of[2], (SAMPLES,), 0, ENVS), jax.random.fold_in(streams_of[2], 1), 0, ENVS - 1).astype(jnp.int32),
        "variances": jnp.clip(jnp.exp(jax.random.uniform(streams_of[3], (3,), jnp.float32, math.log(0.25), math.log(1.0))), 0.25, 1.0),
    }


def apply_operator(current, genotypes, onehot, variances):
    rounded = current.astype(jnp.bfloat16)
    scaled = (onehot[:, None, :] * rounded[None, :, :]).reshape(ENVS * PROBES, -1)
    panel = jnp.concatenate([rounded, scaled], axis=0)
    snp_panel = jnp.dot(panel, genotypes, preferred_element_type=jnp.float32).astype(jnp.bfloat16)
    image = lax.dot_general(snp_panel, genotypes, (((1,), (1,)), ((), ())), preferred_element_type=jnp.float32)
    additive = image[:PROBES]
    blocks = image[PROBES:].reshape(ENVS, PROBES, -1)
    interaction = jnp.sum(onehot.astype(jnp.float32)[:, None, :] * blocks, axis=0)
    return variances[0] * additive / SNPS + variances[1] * interaction / SNPS + variances[2] * current


def reference(genotypes, probes, env_label, variances):
    labels = jnp.arange(ENVS, dtype=jnp.int32)
    onehot = (env_label[None, :] == labels[:, None]).astype(jnp.bfloat16)
    first = apply_operator(probes.astype(jnp.float32), genotypes, onehot, variances)
    second = apply_operator(first, genotypes, onehot, variances)
    return first, second
```

```python
import jax
import jax.numpy as jnp
from jax import lax
from jax.sharding import PartitionSpec as P

ENVS = 8


def exchange(block, offset, devices):
    return lax.ppermute(block, "samp", [(k, k ^ offset) for k in range(devices)])


def make(mesh):
    samp = mesh.shape["samp"]
    snp = mesh.shape["snp"]
    chips = samp // 2

    def block_of(array, index, width):
        return lax.dynamic_slice_in_dim(array, index * width, width, axis=1)

    def apply_operator(current, genotypes, onehot, scale, noise, exact):
        probes = current.shape[0]
        wire = jnp.float32 if exact else jnp.bfloat16
        snps = genotypes.shape[1]
        half, width = snps // 2, snps // samp
        index = lax.axis_index("samp")
        core, chip = index % 2, index // 2
        rounded = current.astype(jnp.bfloat16)
        panel = (onehot[:, None, :] * rounded[None, :, :]).reshape(ENVS * probes, -1)
        partial = jnp.dot(panel, genotypes, preferred_element_type=jnp.float32)
        given = exchange(block_of(partial, 1 - core, half).astype(wire), 1, samp)
        pair = block_of(partial, core, half) + given.astype(jnp.float32)
        total = block_of(pair, chip, width)
        for step in range(1, chips):
            total = total + exchange(block_of(pair, chip ^ step, width).astype(wire), 2 * step, samp).astype(jnp.float32)
        if exact:
            total = jnp.concatenate([total.reshape(ENVS, probes, width).sum(0), total], axis=0)
        mine = total.astype(jnp.bfloat16)
        rows = mine.shape[0]
        gathered = jnp.zeros((rows, half), jnp.bfloat16)
        for step in range(chips):
            piece = exchange(mine, 2 * step, samp) if step else mine
            gathered = lax.dynamic_update_slice(gathered, piece, (0, (chip ^ step) * width))
        other = exchange(gathered, 1, samp)
        dims = (((1,), (1,)), ((), ()))
        image = lax.dot_general(gathered, block_of(genotypes, core, half), dims, preferred_element_type=jnp.float32)
        image = image + lax.dot_general(other, block_of(genotypes, 1 - core, half), dims, preferred_element_type=jnp.float32)
        blocks = image[rows - ENVS * probes:].reshape(ENVS, probes, -1)
        if exact:
            weight = scale[1] * onehot.astype(jnp.float32)
            weighted = scale[0] * image[:probes] + jnp.sum(weight[:, None, :] * blocks, axis=0)
        else:
            weight = scale[0] + scale[1] * onehot.astype(jnp.float32)
            weighted = jnp.sum(weight[:, None, :] * blocks, axis=0)
        parts = [weighted] + [
            lax.ppermute(weighted, "snp", [(k, k ^ step) for k in range(snp)]) for step in range(1, snp)
        ]
        while len(parts) > 1:
            parts = [parts[k] + parts[k + 1] for k in range(0, len(parts), 2)]
        return parts[0] + noise * current

    def per_device(genotypes, probes, env_label, variances):
        total_snps = genotypes.shape[1] * snp
        labels = jnp.arange(ENVS, dtype=jnp.int32)
        onehot = (env_label[None, :] == labels[:, None]).astype(jnp.bfloat16)
        scale = variances[:2] / total_snps
        first = apply_operator(probes.astype(jnp.float32), genotypes, onehot, scale, variances[2], True)
        second = apply_operator(first, genotypes, onehot, scale, variances[2], False)
        return (first, second)

    return per_device


def solution(mesh):
    return jax.shard_map(
        make(mesh),
        mesh=mesh,
        in_specs=(P("samp", "snp"), P(None, "samp"), P("samp"), P()),
        out_specs=(P(None, "samp"), P(None, "samp")),
        check_vma=False,
    )
```

```python
import functools

import jax
import jax.numpy as jnp
from jax import lax
from jax.experimental import pallas as pl
from jax.experimental.pallas import tpu as pltpu
from jax.sharding import PartitionSpec as P

ENVS = 8
VMEM = pl.BlockSpec(memory_space=pltpu.VMEM)
SMEM = pl.BlockSpec(memory_space=pltpu.SMEM)
HBM = pl.BlockSpec(memory_space=pltpu.HBM)
LIMIT = 24 * 1024 * 1024


def build_panel(rounded, labels):
    rows = [jnp.where(labels == e, rounded, 0.0) for e in range(ENVS)]
    return jnp.concatenate(rows, axis=0).astype(jnp.bfloat16)


def load_body(place, probes, labels, genotypes, held, partial, sems, *, other):
    chips, _, width = held.shape
    core, chip = place[0], place[1]
    half = (1 - core) if other else core

    def copy(d):
        start = pl.multiple_of((half * chips + (chip ^ d)) * width, width)
        return pltpu.make_async_copy(genotypes.at[:, pl.ds(start, width)], held.at[d], sems.at[d])

    ahead = min(2, chips)
    for d in range(ahead):
        copy(d).start()
    panel = build_panel(probes[...].astype(jnp.float32), labels[...])
    for d in range(chips):
        copy(d).wait()
        if d + ahead < chips:
            copy(d + ahead).start()
        partial[:, pl.ds(d * width, width)] = jnp.dot(
            panel, held[d], preferred_element_type=jnp.float32
        ).astype(partial.dtype)


def load_half(place, probes, labels, genotypes, chips, width, other, wire):
    samples = probes.shape[1]
    rows = ENVS * probes.shape[0]
    return pl.pallas_call(
        functools.partial(load_body, other=other),
        in_specs=[SMEM, VMEM, VMEM, HBM],
        out_specs=(VMEM, VMEM),
        out_shape=(
            pltpu.VMEM((chips, samples, width), genotypes.dtype),
            jax.ShapeDtypeStruct((rows, chips * width), wire),
        ),
        scratch_shapes=[pltpu.SemaphoreType.DMA((chips,))],
        compiler_params=pltpu.CompilerParams(vmem_limit_bytes=LIMIT),
        name="load_other" if other else "load_own",
    )(place, probes, labels, genotypes)


def step_body(noise, current, labels, held, *refs, count):
    parts = [refs[k][...] for k in range(count)]
    first, panel_out, partial = refs[count:]
    while len(parts) > 1:
        parts = [parts[k] + parts[k + 1] for k in range(0, len(parts), 2)]
    value = parts[0] + noise[2] * current[...].astype(jnp.float32)
    first[...] = value
    panel = build_panel(value.astype(jnp.bfloat16).astype(jnp.float32), labels[...])
    panel_out[...] = panel
    width = held.shape[2]
    for d in range(held.shape[0]):
        partial[:, pl.ds(d * width, width)] = jnp.dot(
            panel, held[d], preferred_element_type=jnp.float32
        ).astype(partial.dtype)


def step_half(variances, current, labels, held, parts, wire):
    rows = ENVS * current.shape[0]
    chips, samples, width = held.shape
    return pl.pallas_call(
        functools.partial(step_body, count=len(parts)),
        in_specs=[SMEM] + [VMEM] * (3 + len(parts)),
        out_specs=(VMEM, VMEM, VMEM),
        out_shape=(
            jax.ShapeDtypeStruct(current.shape, jnp.float32),
            jax.ShapeDtypeStruct((rows, samples), jnp.bfloat16),
            jax.ShapeDtypeStruct((rows, chips * width), wire),
        ),
        compiler_params=pltpu.CompilerParams(vmem_limit_bytes=LIMIT),
        name="step_other",
    )(variances, current, labels, held, *parts)


def panel_body(panel, held, partial):
    width = held.shape[2]
    for d in range(held.shape[0]):
        partial[:, pl.ds(d * width, width)] = jnp.dot(panel[...], held[d], preferred_element_type=jnp.float32)


def panel_half(panel, held):
    chips, _, width = held.shape
    return pl.pallas_call(
        panel_body,
        in_specs=[VMEM, VMEM],
        out_specs=VMEM,
        out_shape=jax.ShapeDtypeStruct((panel.shape[0], chips * width), jnp.float32),
        compiler_params=pltpu.CompilerParams(vmem_limit_bytes=LIMIT),
        name="step_own",
    )(panel, held)


def dot_t(a, b):
    return lax.dot_general(a, b, (((1,), (1,)), ((), ())), preferred_element_type=jnp.float32)


def image_body(panel, held, image):
    width = held.shape[2]
    total = dot_t(panel[:, pl.ds(0, width)], held[0])
    for d in range(1, held.shape[0]):
        total += dot_t(panel[:, pl.ds(d * width, width)], held[d])
    image[...] = total


def image_half(panel, held):
    return pl.pallas_call(
        image_body,
        in_specs=[VMEM, VMEM],
        out_specs=VMEM,
        out_shape=jax.ShapeDtypeStruct((panel.shape[0], held.shape[1]), jnp.float32),
        compiler_params=pltpu.CompilerParams(vmem_limit_bytes=LIMIT),
        name="image_own",
    )(panel, held)


def finish_body(variances, labels, panel, held, image, weighted, *, snps, exact):
    width = held.shape[2]
    total = image[...]
    for d in range(held.shape[0]):
        total += dot_t(panel[:, pl.ds(d * width, width)], held[d])
    probes = weighted.shape[0]
    additive, interaction = variances[0] * (1.0 / snps), variances[1] * (1.0 / snps)
    tag = labels[...]
    skip = probes if exact else 0
    result = additive * total[:probes] if exact else None
    for e in range(ENVS):
        block = total[skip + e * probes : skip + (e + 1) * probes]
        scale = jnp.where(tag == e, interaction, 0.0) + (0.0 if exact else additive)
        term = scale * block
        result = term if result is None else result + term
    weighted[...] = result


def finish_half(variances, labels, panel, held, image, probes, snps, exact):
    return pl.pallas_call(
        functools.partial(finish_body, snps=snps, exact=exact),
        in_specs=[SMEM, VMEM, VMEM, VMEM, VMEM],
        out_specs=VMEM,
        out_shape=jax.ShapeDtypeStruct((probes, held.shape[1]), jnp.float32),
        compiler_params=pltpu.CompilerParams(vmem_limit_bytes=LIMIT),
        name="image_other",
    )(variances, labels, panel, held, image)


def make(mesh):
    samp, snp = mesh.shape["samp"], mesh.shape["snp"]
    chips = samp // 2

    def exchange(block, offset):
        return lax.ppermute(block, "samp", [(k, k ^ offset) for k in range(samp)])

    def reduce_panel(given, own, wire, probes, exact):
        width = own.shape[1] // chips
        pair = own + exchange(given, 1).astype(jnp.float32)
        total = pair[:, :width]
        for step in range(1, chips):
            block = pair[:, step * width : (step + 1) * width].astype(wire)
            total = total + exchange(block, 2 * step).astype(jnp.float32)
        if exact:
            total = jnp.concatenate([total.reshape(ENVS, probes, width).sum(0), total], axis=0)
        return total.astype(jnp.bfloat16)

    def gather_panel(mine):
        return jnp.concatenate([mine] + [exchange(mine, 2 * step) for step in range(1, chips)], axis=1)

    def per_device(genotypes, probes, env_label, variances):
        snps = genotypes.shape[1] * snp
        count = probes.shape[0]
        width = genotypes.shape[1] // samp
        index = lax.axis_index("samp")
        place = jnp.stack([index % 2, index // 2]).astype(jnp.int32)
        labels = env_label[None, :]

        def image_of(panel, exact):
            other = exchange(panel, 1)
            image = image_half(panel, held_own)
            return finish_half(variances, labels, other, held_other, image, count, snps, exact)

        def spread(weighted):
            return [weighted] + [
                lax.ppermute(weighted, "snp", [(k, k ^ step) for k in range(snp)]) for step in range(1, snp)
            ]

        held_other, given = load_half(place, probes, labels, genotypes, chips, width, True, jnp.float32)
        held_own, own = load_half(place, probes, labels, genotypes, chips, width, False, jnp.float32)
        panel = gather_panel(reduce_panel(given, own, jnp.float32, count, True))
        parts = spread(image_of(panel, True))
        first, scaled, given = step_half(variances, probes, labels, held_other, parts, jnp.bfloat16)
        own = panel_half(scaled, held_own)
        panel = gather_panel(reduce_panel(given, own, jnp.bfloat16, count, False))
        parts = spread(image_of(panel, False))
        while len(parts) > 1:
            parts = [parts[k] + parts[k + 1] for k in range(0, len(parts), 2)]
        return (first, parts[0] + variances[2] * first)

    return per_device


def solution(mesh):
    return jax.shard_map(
        make(mesh),
        mesh=mesh,
        in_specs=(P("samp", "snp"), P(None, "samp"), P("samp"), P()),
        out_specs=(P(None, "samp"), P(None, "samp")),
        check_vma=False,
    )
```

```python
import functools

import jax
import jax.numpy as jnp
from jax import lax
from jax.experimental import pallas as pl
from jax.experimental.pallas import tpu as pltpu
from jax.sharding import PartitionSpec as P

ENVS = 8
VMEM = pl.BlockSpec(memory_space=pltpu.VMEM)
SMEM = pl.BlockSpec(memory_space=pltpu.SMEM)
HBM = pl.BlockSpec(memory_space=pltpu.HBM)
LIMIT = 24 * 1024 * 1024


def build_panel(rounded, labels):
    rows = [jnp.where(labels == e, rounded, 0.0) for e in range(ENVS)]
    return jnp.concatenate(rows, axis=0).astype(jnp.bfloat16)


def load_body(place, probes, labels, genotypes, *refs, first):
    if first:
        held, partial, panel, probes_in, labels_in, sems, small = refs
    else:
        held, partial, sems = refs
    chips, _, width = held.shape
    half = (1 - place[0]) if first else place[0]

    def copy(d):
        start = pl.multiple_of((half * chips + (place[1] ^ d)) * width, width)
        return pltpu.make_async_copy(genotypes.at[:, pl.ds(start, width)], held.at[d], sems.at[d])

    if first:
        inputs = (
            pltpu.make_async_copy(probes, probes_in, small.at[0]),
            pltpu.make_async_copy(labels, labels_in, small.at[1]),
        )
        for move in inputs:
            move.start()
    ahead = min(2, chips)
    for d in range(ahead):
        copy(d).start()
    if first:
        for move in inputs:
            move.wait()
        panel[...] = build_panel(probes_in[...].astype(jnp.float32), labels_in[...])
    else:
        panel = probes
    for d in range(chips):
        copy(d).wait()
        if d + ahead < chips:
            copy(d + ahead).start()
        partial[:, pl.ds(d * width, width)] = jnp.dot(panel[...], held[d], preferred_element_type=jnp.float32)


def load_first(place, probes, labels, genotypes, chips, width):
    count, samples = probes.shape
    rows = ENVS * count
    return pl.pallas_call(
        functools.partial(load_body, first=True),
        in_specs=[SMEM, HBM, HBM, HBM],
        out_specs=(VMEM,) * 5,
        out_shape=(
            pltpu.VMEM((chips, samples, width), genotypes.dtype),
            jax.ShapeDtypeStruct((rows, chips * width), jnp.float32),
            jax.ShapeDtypeStruct((rows, samples), jnp.bfloat16),
            pltpu.VMEM(probes.shape, probes.dtype),
            pltpu.VMEM(labels.shape, labels.dtype),
        ),
        scratch_shapes=[pltpu.SemaphoreType.DMA((chips,)), pltpu.SemaphoreType.DMA((2,))],
        compiler_params=pltpu.CompilerParams(vmem_limit_bytes=LIMIT),
        name="load_other",
    )(place, probes, labels, genotypes)


def load_second(place, panel, labels, genotypes, chips, width):
    rows, samples = panel.shape
    return pl.pallas_call(
        functools.partial(load_body, first=False),
        in_specs=[SMEM, VMEM, VMEM, HBM],
        out_specs=(VMEM, VMEM),
        out_shape=(
            pltpu.VMEM((chips, samples, width), genotypes.dtype),
            jax.ShapeDtypeStruct((rows, chips * width), jnp.float32),
        ),
        scratch_shapes=[pltpu.SemaphoreType.DMA((chips,))],
        compiler_params=pltpu.CompilerParams(vmem_limit_bytes=LIMIT),
        name="load_own",
    )(place, panel, labels, genotypes)


def step_body(noise, current, labels, held, *refs, count):
    parts = [refs[k][...] for k in range(count)]
    first, noise_term, panel_out, partial = refs[count:]
    while len(parts) > 1:
        parts = [parts[k] + parts[k + 1] for k in range(0, len(parts), 2)]
    value = parts[0] + noise[2] * current[...].astype(jnp.float32)
    first[...] = value
    noise_term[...] = noise[2] * value
    panel = build_panel(value.astype(jnp.bfloat16).astype(jnp.float32), labels[...])
    panel_out[...] = panel
    width = held.shape[2]
    for d in range(held.shape[0]):
        partial[:, pl.ds(d * width, width)] = jnp.dot(
            panel, held[d], preferred_element_type=jnp.float32
        ).astype(partial.dtype)


def step_half(variances, current, labels, held, parts, wire):
    rows = ENVS * current.shape[0]
    chips, samples, width = held.shape
    return pl.pallas_call(
        functools.partial(step_body, count=len(parts)),
        in_specs=[SMEM] + [VMEM] * (3 + len(parts)),
        out_specs=(VMEM,) * 4,
        out_shape=(
            pltpu.VMEM(current.shape, jnp.float32),
            pltpu.VMEM(current.shape, jnp.float32),
            jax.ShapeDtypeStruct((rows, samples), jnp.bfloat16),
            jax.ShapeDtypeStruct((rows, chips * width), wire),
        ),
        compiler_params=pltpu.CompilerParams(vmem_limit_bytes=LIMIT),
        name="step_other",
    )(variances, current, labels, held, *parts)


def panel_body(panel, held, partial):
    width = held.shape[2]
    for d in range(held.shape[0]):
        partial[:, pl.ds(d * width, width)] = jnp.dot(panel[...], held[d], preferred_element_type=jnp.float32)


def panel_half(panel, held):
    chips, _, width = held.shape
    return pl.pallas_call(
        panel_body,
        in_specs=[VMEM, VMEM],
        out_specs=VMEM,
        out_shape=jax.ShapeDtypeStruct((panel.shape[0], chips * width), jnp.float32),
        compiler_params=pltpu.CompilerParams(vmem_limit_bytes=LIMIT),
        name="step_own",
    )(panel, held)


def dot_t(a, b):
    return lax.dot_general(a, b, (((1,), (1,)), ((), ())), preferred_element_type=jnp.float32)


def image_body(panel, held, image):
    width = held.shape[2]
    total = dot_t(panel[:, pl.ds(0, width)], held[0])
    for d in range(1, held.shape[0]):
        total += dot_t(panel[:, pl.ds(d * width, width)], held[d])
    image[...] = total


def image_half(panel, held):
    return pl.pallas_call(
        image_body,
        in_specs=[VMEM, VMEM],
        out_specs=VMEM,
        out_shape=jax.ShapeDtypeStruct((panel.shape[0], held.shape[1]), jnp.float32),
        compiler_params=pltpu.CompilerParams(vmem_limit_bytes=LIMIT),
        name="image_own",
    )(panel, held)


def finish_body(variances, labels, panel, held, image, weighted, *, snps, exact):
    width = held.shape[2]
    total = image[...]
    for d in range(held.shape[0]):
        total += dot_t(panel[:, pl.ds(d * width, width)], held[d])
    probes = weighted.shape[0]
    additive, interaction = variances[0] * (1.0 / snps), variances[1] * (1.0 / snps)
    tag = labels[...]
    skip = probes if exact else 0
    result = additive * total[:probes] if exact else None
    for e in range(ENVS):
        block = total[skip + e * probes : skip + (e + 1) * probes]
        scale = jnp.where(tag == e, interaction, 0.0) + (0.0 if exact else additive)
        term = scale * block
        result = term if result is None else result + term
    weighted[...] = result


def finish_half(variances, labels, panel, held, image, probes, snps, exact):
    return pl.pallas_call(
        functools.partial(finish_body, snps=snps, exact=exact),
        in_specs=[SMEM, VMEM, VMEM, VMEM, VMEM],
        out_specs=VMEM,
        out_shape=jax.ShapeDtypeStruct((probes, held.shape[1]), jnp.float32),
        compiler_params=pltpu.CompilerParams(vmem_limit_bytes=LIMIT),
        name="image_other",
    )(variances, labels, panel, held, image)


def make(mesh):
    samp, snp = mesh.shape["samp"], mesh.shape["snp"]
    chips = samp // 2

    far = sorted(range(1, chips), key=lambda step: -bin(step).count("1"))

    def exchange(block, offset):
        return lax.ppermute(block, "samp", [(k, k ^ offset) for k in range(samp)])

    def reduce_panel(given, own, wire, probes, exact):
        width = own.shape[1] // chips
        pair = own + exchange(given, 1).astype(jnp.float32)
        total = pair[:, :width]
        for step in far:
            block = pair[:, step * width : (step + 1) * width].astype(wire)
            total = total + exchange(block, 2 * step + step % 2).astype(jnp.float32)
        if exact:
            total = jnp.concatenate([total.reshape(ENVS, probes, width).sum(0), total], axis=0)
        return total.astype(jnp.bfloat16)

    def gather_panel(mine):
        pieces = {step: exchange(mine, 2 * step + step % 2) for step in far}
        return jnp.concatenate([mine] + [pieces[step] for step in range(1, chips)], axis=1)

    def per_device(genotypes, probes, env_label, variances):
        snps = genotypes.shape[1] * snp
        count = probes.shape[0]
        width = genotypes.shape[1] // samp
        index = lax.axis_index("samp")
        core, chip = index & 1, index >> 1
        place = jnp.stack([core ^ (chip & 1), chip]).astype(jnp.int32)
        labels = env_label[None, :]
        genotypes, probes, labels = (pltpu.with_memory_space_constraint(a, pltpu.HBM) for a in (genotypes, probes, labels))

        def image_of(panel, exact):
            other = exchange(panel, 1)
            image = image_half(panel, held_own)
            return finish_half(variances, labels, other, held_other, image, count, snps, exact)

        def spread(weighted):
            pieces = {
                step: lax.ppermute(weighted, "snp", [(k, k ^ step) for k in range(snp)])
                for step in range(snp - 1, 0, -1)
            }
            return [weighted] + [pieces[step] for step in range(1, snp)]

        held_other, given, scaled, current, labels = load_first(place, probes, labels, genotypes, chips, width)
        held_own, own = load_second(place, scaled, labels, genotypes, chips, width)
        panel = gather_panel(reduce_panel(given, own, jnp.float32, count, True))
        parts = spread(image_of(panel, True))
        first, noise, scaled, given = step_half(variances, current, labels, held_other, parts, jnp.bfloat16)
        own = panel_half(scaled, held_own)
        panel = gather_panel(reduce_panel(given, own, jnp.bfloat16, count, False))
        parts = spread(image_of(panel, False))
        while len(parts) > 1:
            parts = [parts[k] + parts[k + 1] for k in range(0, len(parts), 2)]
        return (first, parts[0] + noise)

    return per_device


def solution(mesh):
    return jax.shard_map(
        make(mesh),
        mesh=mesh,
        in_specs=(P("samp", "snp"), P(None, "samp"), P("samp"), P()),
        out_specs=(P(None, "samp"), P(None, "samp")),
        check_vma=False,
    )
```

```python
import functools

import jax
import jax.numpy as jnp
from jax import lax
from jax.experimental import pallas as pl
from jax.experimental.pallas import tpu as pltpu
from jax.sharding import PartitionSpec as P


ENVS = 8
VMEM = pl.BlockSpec(memory_space=pltpu.VMEM)
HBM = pl.BlockSpec(memory_space=pltpu.HBM)
PARAMS = pltpu.CompilerParams(vmem_limit_bytes=24 * 1024 * 1024)
f32 = jnp.float32


def build_panel(rounded, tags):
    rows = [jnp.where(tags == e, rounded, 0.0) for e in range(ENVS)]
    return jnp.concatenate(rows, axis=0).astype(jnp.bfloat16)


def dot_t(a, b):
    return lax.dot_general(a, b, (((1,), (1,)), ((), ())), preferred_element_type=f32)


def copies(genotypes, held, sems, other):
    chips, _, width = held.shape
    index = lax.axis_index("samp")
    core, chip = index & 1, index >> 1
    half = core ^ (chip & 1)
    if other:
        half = 1 - half

    def copy(d):
        start = pl.multiple_of((half * chips + (chip ^ d)) * width, width)
        return pltpu.make_async_copy(genotypes.at[:, pl.ds(start, width)], held.at[d], sems.at[d])

    return [copy(d) for d in range(chips)]


def products(panel, held, partial):
    width = held.shape[2]
    for d in range(held.shape[0]):
        partial[:, pl.ds(d * width, width)] = jnp.dot(panel, held[d], preferred_element_type=f32).astype(partial.dtype)


def first_body(probes, labels, variances, genotypes, held, partial, panel, current, tags, scales, labels_in, numbers, sems, small, *, snps):
    moves = copies(genotypes, held, sems, True)
    inputs = (
        pltpu.make_async_copy(probes, current, small.at[0]),
        pltpu.make_async_copy(labels, labels_in, small.at[1]),
        pltpu.make_async_copy(variances, numbers, small.at[2]),
    )
    for move in inputs:
        move.start()
    for move in moves:
        move.start()
    for move in inputs:
        move.wait()
    tag = jnp.broadcast_to(labels_in[...], tags.shape)
    tags[...] = tag
    built = build_panel(current[...].astype(f32), tag)
    panel[...] = built
    shape = scales.shape[1:]
    scales[0] = jnp.full(shape, numbers[0] * (1.0 / snps), f32)
    scales[1] = jnp.full(shape, numbers[1] * (1.0 / snps), f32)
    scales[2] = jnp.full(shape, numbers[2], f32)
    width = held.shape[2]
    for d, move in enumerate(moves):
        move.wait()
        partial[:, pl.ds(d * width, width)] = jnp.dot(built, held[d], preferred_element_type=f32)


def load_first(probes, labels, variances, genotypes, chips, width, snps):
    count, samples = probes.shape
    rows = ENVS * count
    return pl.pallas_call(
        functools.partial(first_body, snps=snps),
        in_specs=[HBM] * 4,
        out_specs=(VMEM,) * 6,
        out_shape=(
            pltpu.VMEM((chips, samples, width), genotypes.dtype),
            pltpu.VMEM((rows, chips * width), f32),
            pltpu.VMEM((rows, samples), jnp.bfloat16),
            pltpu.VMEM(probes.shape, probes.dtype),
            pltpu.VMEM(probes.shape, jnp.int32),
            pltpu.VMEM((3,) + probes.shape, f32),
        ),
        scratch_shapes=[
            pltpu.VMEM(labels.shape, labels.dtype),
            pltpu.SMEM(variances.shape, variances.dtype),
            pltpu.SemaphoreType.DMA((chips,)),
            pltpu.SemaphoreType.DMA((3,)),
        ],
        compiler_params=PARAMS,
        name="load_other",
    )(probes, labels, variances, genotypes)


def second_body(panel, genotypes, held, partial, sems):
    moves = copies(genotypes, held, sems, False)
    for move in moves:
        move.start()
    width = held.shape[2]
    for d, move in enumerate(moves):
        move.wait()
        partial[:, pl.ds(d * width, width)] = jnp.dot(panel[...], held[d], preferred_element_type=f32)


def load_second(panel, genotypes, chips, width):
    rows, samples = panel.shape
    return pl.pallas_call(
        second_body,
        in_specs=[VMEM, HBM],
        out_specs=(VMEM, VMEM),
        out_shape=(
            pltpu.VMEM((chips, samples, width), genotypes.dtype),
            pltpu.VMEM((rows, chips * width), f32),
        ),
        scratch_shapes=[pltpu.SemaphoreType.DMA((chips,))],
        compiler_params=PARAMS,
        name="load_own",
    )(panel, genotypes)


def tree_sum(parts):
    while len(parts) > 1:
        parts = [parts[k] + parts[k + 1] for k in range(0, len(parts), 2)]
    return parts[0]


def step_body(current, tags, scales, held, *refs, count):
    first, noise, panel, partial = refs[count:]
    value = tree_sum([refs[k][...] for k in range(count)]) + scales[2] * current[...].astype(f32)
    first[...] = value
    noise[...] = scales[2] * value
    built = build_panel(value.astype(jnp.bfloat16).astype(f32), tags[...])
    panel[...] = built
    products(built, held, partial)


def step_half(current, tags, scales, held, parts, wire):
    rows = ENVS * current.shape[0]
    chips, samples, width = held.shape
    return pl.pallas_call(
        functools.partial(step_body, count=len(parts)),
        in_specs=[VMEM] * (4 + len(parts)),
        out_specs=(VMEM,) * 4,
        out_shape=(
            pltpu.VMEM(current.shape, f32),
            pltpu.VMEM(current.shape, f32),
            pltpu.VMEM((rows, samples), jnp.bfloat16),
            pltpu.VMEM((rows, chips * width), wire),
        ),
        compiler_params=PARAMS,
        name="step_other",
    )(current, tags, scales, held, *parts)


def panel_body(panel, held, partial):
    products(panel[...], held, partial)


def panel_half(panel, held):
    chips, _, width = held.shape
    return pl.pallas_call(
        panel_body,
        in_specs=[VMEM, VMEM],
        out_specs=VMEM,
        out_shape=pltpu.VMEM((panel.shape[0], chips * width), f32),
        compiler_params=PARAMS,
        name="step_own",
    )(panel, held)


def image_body(*refs, blocks, pieces, more, probes):
    panels, refs = refs[:pieces], refs[pieces:]
    held, refs = refs[0], refs[1:]
    width = held.shape[2]
    total = None
    if more:
        total, refs = refs[0][...], refs[1:]
    for k, d in enumerate(blocks):
        per = panels[0].shape[1] // width
        part = panels[k // per][:, pl.ds((k % per) * width, width)]
        term = dot_t(part, held[d])
        total = term if total is None else total + term
    if probes is None:
        refs[0][...] = total
        return
    tags, scales, weighted = refs
    exact = total.shape[0] > ENVS * probes
    tag, additive, interaction = tags[...], scales[0], scales[1]
    skip = probes if exact else 0
    low = jnp.zeros_like(additive) if exact else additive
    high = interaction if exact else additive + interaction
    result = additive * total[:probes] if exact else None
    for e in range(ENVS):
        term = jnp.where(tag == e, high, low) * total[skip + e * probes : skip + (e + 1) * probes]
        result = term if result is None else result + term
    weighted[...] = result


def image(panels, held, blocks, before=None, finish=None):
    rows, samples = panels[0].shape[0], held.shape[1]
    operands = list(panels) + [held] + ([before] if before is not None else [])
    probes = None
    out = pltpu.VMEM((rows, samples), f32)
    if finish is not None:
        operands += list(finish)
        probes = finish[0].shape[0]
        out = pltpu.VMEM(finish[0].shape, f32)
    return pl.pallas_call(
        functools.partial(image_body, blocks=tuple(blocks), pieces=len(panels), more=before is not None, probes=probes),
        in_specs=[VMEM] * len(operands),
        out_specs=VMEM,
        out_shape=out,
        compiler_params=PARAMS,
        name="image",
    )(*operands)


def make(mesh):
    samp, snp = mesh.shape["samp"], mesh.shape["snp"]
    chips = samp // 2
    far = sorted(range(1, chips), key=lambda step: -bin(step).count("1"))
    early = [0] + far[: chips // 2 - 1]
    late = far[chips // 2 - 1 :]

    def exchange(block, offset):
        return lax.ppermute(block, "samp", [(k, k ^ offset) for k in range(samp)])

    def between(block, step):
        return exchange(block, 2 * step + step % 2)

    def reduce_panel(given, own, wire, probes, exact):
        width = own.shape[1] // chips
        pair = own + exchange(given, 1).astype(f32)
        total = pair[:, :width]
        for step in far:
            total = total + between(pair[:, step * width : (step + 1) * width].astype(wire), step).astype(f32)
        if exact:
            total = jnp.concatenate([total.reshape(ENVS, probes, width).sum(0), total], axis=0)
        return total.astype(jnp.bfloat16)

    def spread_image(mine, held_own, held_other, finish):
        pieces = {0: mine}
        for step in far:
            pieces[step] = between(mine, step)
        early_pieces = [pieces[d] for d in early]
        late_pieces = [pieces[d] for d in late]
        early_other = exchange(jnp.concatenate(early_pieces, axis=1), 1)
        late_other = exchange(jnp.concatenate(late_pieces, axis=1), 1)
        total = image([mine], held_own, [0])
        total = image(early_pieces[1:], held_own, early[1:], total)
        total = image([early_other], held_other, early, total)
        total = image(late_pieces, held_own, late, total)
        return image([late_other], held_other, late, total, finish)

    def per_device(genotypes, probes, env_label, variances):
        snps = genotypes.shape[1] * snp
        count = probes.shape[0]
        width = genotypes.shape[1] // samp
        inputs = (genotypes, probes, env_label[None, :], variances)
        genotypes, probes, labels, variances = (pltpu.with_memory_space_constraint(a, pltpu.HBM) for a in inputs)

        def spread(weighted):
            pieces = {
                step: lax.ppermute(weighted, "snp", [(k, k ^ step) for k in range(snp)])
                for step in range(snp - 1, 0, -1)
            }
            return [weighted] + [pieces[step] for step in range(1, snp)]

        held_other, given, panel, current, tags, scales = load_first(probes, labels, variances, genotypes, chips, width, snps)
        held_own, own = load_second(panel, genotypes, chips, width)
        mine = reduce_panel(given, own, f32, count, True)
        parts = spread(spread_image(mine, held_own, held_other, (tags, scales)))
        first, noise, panel, given = step_half(current, tags, scales, held_other, parts, jnp.bfloat16)
        own = panel_half(panel, held_own)
        mine = reduce_panel(given, own, jnp.bfloat16, count, False)
        parts = spread(spread_image(mine, held_own, held_other, (tags, scales)))
        return (first, tree_sum(parts) + noise)

    return per_device


def solution(mesh):
    return jax.shard_map(
        make(mesh),
        mesh=mesh,
        in_specs=(P("samp", "snp"), P(None, "samp"), P("samp"), P()),
        out_specs=(P(None, "samp"), P(None, "samp")),
        check_vma=False,
    )
```

```python
import functools

import jax
import jax.numpy as jnp
from jax import lax
from jax.experimental import pallas as pl
from jax.experimental.pallas import tpu as pltpu
from jax.sharding import PartitionSpec as P


ENVS = 8
VMEM = pl.BlockSpec(memory_space=pltpu.VMEM)
HBM = pl.BlockSpec(memory_space=pltpu.HBM)
PARAMS = pltpu.CompilerParams(vmem_limit_bytes=24 * 1024 * 1024)
f32 = jnp.float32


def build_panel(rounded, tags):
    rows = [jnp.where(tags == e, rounded, 0.0) for e in range(ENVS)]
    return jnp.concatenate(rows, axis=0).astype(jnp.bfloat16)


def dot_t(a, b):
    return lax.dot_general(a, b, (((1,), (1,)), ((), ())), preferred_element_type=f32)


def copies(genotypes, held, sems, other):
    chips, _, width = held.shape
    index = lax.axis_index("samp")
    core, chip = index & 1, index >> 1
    half = core ^ (chip & 1)
    if other:
        half = 1 - half

    def copy(d):
        start = pl.multiple_of((half * chips + (chip ^ d)) * width, width)
        return pltpu.make_async_copy(genotypes.at[:, pl.ds(start, width)], held.at[d], sems.at[d])

    return [copy(d) for d in range(chips)]


def products(panel, held, partial):
    width = held.shape[2]
    for d in range(held.shape[0]):
        partial[:, pl.ds(d * width, width)] = jnp.dot(panel, held[d], preferred_element_type=f32).astype(partial.dtype)


def first_body(probes, labels, variances, genotypes, held, partial, panel, current, tags, scales, labels_in, numbers, sems, small, *, snps):
    moves = copies(genotypes, held, sems, True)
    inputs = (
        pltpu.make_async_copy(probes, current, small.at[0]),
        pltpu.make_async_copy(labels, labels_in, small.at[1]),
        pltpu.make_async_copy(variances, numbers, small.at[2]),
    )
    for move in inputs:
        move.start()
    for move in moves:
        move.start()
    for move in inputs:
        move.wait()
    tag = jnp.broadcast_to(labels_in[...], tags.shape)
    tags[...] = tag
    built = build_panel(current[...].astype(f32), tag)
    panel[...] = built
    shape = scales.shape[1:]
    scales[0] = jnp.full(shape, numbers[0] * (1.0 / snps), f32)
    scales[1] = jnp.full(shape, numbers[1] * (1.0 / snps), f32)
    scales[2] = jnp.full(shape, numbers[2], f32)
    width = held.shape[2]
    for d, move in enumerate(moves):
        move.wait()
        partial[:, pl.ds(d * width, width)] = jnp.dot(built, held[d], preferred_element_type=f32)


def load_first(probes, labels, variances, genotypes, chips, width, snps):
    count, samples = probes.shape
    rows = ENVS * count
    return pl.pallas_call(
        functools.partial(first_body, snps=snps),
        in_specs=[HBM] * 4,
        out_specs=(VMEM,) * 6,
        out_shape=(
            pltpu.VMEM((chips, samples, width), genotypes.dtype),
            pltpu.VMEM((rows, chips * width), f32),
            pltpu.VMEM((rows, samples), jnp.bfloat16),
            pltpu.VMEM(probes.shape, probes.dtype),
            pltpu.VMEM(probes.shape, jnp.int32),
            pltpu.VMEM((3,) + probes.shape, f32),
        ),
        scratch_shapes=[
            pltpu.VMEM(labels.shape, labels.dtype),
            pltpu.SMEM(variances.shape, variances.dtype),
            pltpu.SemaphoreType.DMA((chips,)),
            pltpu.SemaphoreType.DMA((3,)),
        ],
        compiler_params=PARAMS,
        name="load_other",
    )(probes, labels, variances, genotypes)


def second_body(panel, genotypes, held, partial, sems):
    moves = copies(genotypes, held, sems, False)
    for move in moves:
        move.start()
    width = held.shape[2]
    for d, move in enumerate(moves):
        move.wait()
        partial[:, pl.ds(d * width, width)] = jnp.dot(panel[...], held[d], preferred_element_type=f32)


def load_second(panel, genotypes, chips, width):
    rows, samples = panel.shape
    return pl.pallas_call(
        second_body,
        in_specs=[VMEM, HBM],
        out_specs=(VMEM, VMEM),
        out_shape=(
            pltpu.VMEM((chips, samples, width), genotypes.dtype),
            pltpu.VMEM((rows, chips * width), f32),
        ),
        scratch_shapes=[pltpu.SemaphoreType.DMA((chips,))],
        compiler_params=PARAMS,
        name="load_own",
    )(panel, genotypes)


def tree_sum(parts):
    while len(parts) > 1:
        parts = [parts[k] + parts[k + 1] for k in range(0, len(parts), 2)]
    return parts[0]


def step_body(current, tags, scales, held, *refs, count):
    first, noise, panel, partial = refs[count:]
    value = tree_sum([refs[k][...] for k in range(count)]) + scales[2] * current[...].astype(f32)
    first[...] = value
    noise[...] = scales[2] * value
    built = build_panel(value.astype(jnp.bfloat16).astype(f32), tags[...])
    panel[...] = built
    products(built, held, partial)


def step_half(current, tags, scales, held, parts, wire):
    rows = ENVS * current.shape[0]
    chips, samples, width = held.shape
    return pl.pallas_call(
        functools.partial(step_body, count=len(parts)),
        in_specs=[VMEM] * (4 + len(parts)),
        out_specs=(VMEM,) * 4,
        out_shape=(
            pltpu.VMEM(current.shape, f32),
            pltpu.VMEM(current.shape, f32),
            pltpu.VMEM((rows, samples), jnp.bfloat16),
            pltpu.VMEM((rows, chips * width), wire),
        ),
        compiler_params=PARAMS,
        name="step_other",
    )(current, tags, scales, held, *parts)


def panel_body(panel, held, partial):
    products(panel[...], held, partial)


def panel_half(panel, held):
    chips, _, width = held.shape
    return pl.pallas_call(
        panel_body,
        in_specs=[VMEM, VMEM],
        out_specs=VMEM,
        out_shape=pltpu.VMEM((panel.shape[0], chips * width), f32),
        compiler_params=PARAMS,
        name="step_own",
    )(panel, held)


def image_body(*refs, blocks, pieces, more, probes):
    panels, refs = refs[:pieces], refs[pieces:]
    held, refs = refs[0], refs[1:]
    width = held.shape[2]
    total = None
    if more:
        total, refs = refs[0][...], refs[1:]
    for k, d in enumerate(blocks):
        per = panels[0].shape[1] // width
        part = panels[k // per][:, pl.ds((k % per) * width, width)]
        term = dot_t(part, held[d])
        total = term if total is None else total + term
    if probes is None:
        refs[0][...] = total
        return
    tags, scales, weighted = refs
    exact = total.shape[0] > ENVS * probes
    tag, additive, interaction = tags[...], scales[0], scales[1]
    skip = probes if exact else 0
    low = jnp.zeros_like(additive) if exact else additive
    high = interaction if exact else additive + interaction
    result = additive * total[:probes] if exact else None
    for e in range(ENVS):
        term = jnp.where(tag == e, high, low) * total[skip + e * probes : skip + (e + 1) * probes]
        result = term if result is None else result + term
    weighted[...] = result


def image(panels, held, blocks, before=None, finish=None):
    rows, samples = panels[0].shape[0], held.shape[1]
    operands = list(panels) + [held] + ([before] if before is not None else [])
    probes = None
    out = pltpu.VMEM((rows, samples), f32)
    if finish is not None:
        operands += list(finish)
        probes = finish[0].shape[0]
        out = pltpu.VMEM(finish[0].shape, f32)
    return pl.pallas_call(
        functools.partial(image_body, blocks=tuple(blocks), pieces=len(panels), more=before is not None, probes=probes),
        in_specs=[VMEM] * len(operands),
        out_specs=VMEM,
        out_shape=out,
        compiler_params=PARAMS,
        name="image",
    )(*operands)


def make(mesh):
    samp, snp = mesh.shape["samp"], mesh.shape["snp"]
    chips = samp // 2
    far = sorted(range(1, chips), key=lambda step: -bin(step).count("1"))
    early = far[: chips // 2 - 1]
    late = far[chips // 2 - 1 :]

    def exchange(block, offset):
        return lax.ppermute(block, "samp", [(k, k ^ offset) for k in range(samp)])

    def between(block, step):
        return exchange(block, 2 * step + step % 2)

    def reduce_panel(given, own, wire, probes, exact):
        width = own.shape[1] // chips
        pair = own + exchange(given, 1).astype(f32)
        total = pair[:, :width]
        for step in far:
            total = total + between(pair[:, step * width : (step + 1) * width].astype(wire), step).astype(f32)
        if exact:
            total = jnp.concatenate([total.reshape(ENVS, probes, width).sum(0), total], axis=0)
        return total.astype(jnp.bfloat16)

    def spread_image(mine, held_own, held_other, finish):
        pieces = {}
        for step in far:
            pieces[step] = between(mine, step)
        other = exchange(mine, 1)
        total = image([mine], held_own, [0])
        total = image([other], held_other, [0], total)
        for step in early:
            other = exchange(pieces[step], 1)
            total = image([pieces[step]], held_own, [step], total)
            total = image([other], held_other, [step], total)
        late_pieces = [pieces[step] for step in late]
        other = exchange(jnp.concatenate(late_pieces, axis=1), 1)
        total = image(late_pieces, held_own, late, total)
        return image([other], held_other, late, total, finish)

    def per_device(genotypes, probes, env_label, variances):
        snps = genotypes.shape[1] * snp
        count = probes.shape[0]
        width = genotypes.shape[1] // samp
        inputs = (genotypes, probes, env_label[None, :], variances)
        genotypes, probes, labels, variances = (pltpu.with_memory_space_constraint(a, pltpu.HBM) for a in inputs)

        def spread(weighted):
            pieces = {
                step: lax.ppermute(weighted, "snp", [(k, k ^ step) for k in range(snp)])
                for step in range(snp - 1, 0, -1)
            }
            return [weighted] + [pieces[step] for step in range(1, snp)]

        held_other, given, panel, current, tags, scales = load_first(probes, labels, variances, genotypes, chips, width, snps)
        held_own, own = load_second(panel, genotypes, chips, width)
        mine = reduce_panel(given, own, f32, count, True)
        parts = spread(spread_image(mine, held_own, held_other, (tags, scales)))
        first, noise, panel, given = step_half(current, tags, scales, held_other, parts, jnp.bfloat16)
        own = panel_half(panel, held_own)
        mine = reduce_panel(given, own, jnp.bfloat16, count, False)
        parts = spread(spread_image(mine, held_own, held_other, (tags, scales)))
        return (first, tree_sum(parts) + noise)

    return per_device


def solution(mesh):
    return jax.shard_map(
        make(mesh),
        mesh=mesh,
        in_specs=(P("samp", "snp"), P(None, "samp"), P("samp"), P()),
        out_specs=(P(None, "samp"), P(None, "samp")),
        check_vma=False,
    )
```

```python
import functools

import jax
import jax.numpy as jnp
from jax import lax
from jax.experimental import pallas as pl
from jax.experimental.pallas import tpu as pltpu
from jax.sharding import PartitionSpec as P


ENVS = 8
SCALE_ROWS = 8
VMEM = pl.BlockSpec(memory_space=pltpu.VMEM)
HBM = pl.BlockSpec(memory_space=pltpu.HBM)
PARAMS = pltpu.CompilerParams(vmem_limit_bytes=24 * 1024 * 1024)
f32 = jnp.float32


def build_panel(rounded, tags):
    rows = [jnp.where(tags == e, rounded, 0.0) for e in range(ENVS)]
    return jnp.concatenate(rows, axis=0).astype(jnp.bfloat16)


def dot_t(a, b):
    return lax.dot_general(a, b, (((1,), (1,)), ((), ())), preferred_element_type=f32)


def copies(genotypes, held, sems, other):
    chips, _, width = held.shape
    index = lax.axis_index("samp")
    core, chip = index & 1, index >> 1
    half = core ^ (chip & 1)
    if other:
        half = 1 - half

    def copy(d):
        start = pl.multiple_of((half * chips + (chip ^ d)) * width, width)
        return pltpu.make_async_copy(genotypes.at[:, pl.ds(start, width)], held.at[d], sems.at[d])

    return [copy(d) for d in range(chips)]


def store_bounded(partial, d, block):
    rows, width = block.shape
    partial[pl.ds(0, rows), pl.ds(d * width, width)] = block
    top = jnp.max(jnp.abs(block), axis=0, keepdims=True)
    partial[pl.ds(rows, SCALE_ROWS), pl.ds(d * width, width)] = jnp.broadcast_to(top, (SCALE_ROWS, width))


def products(panel, held, partial):
    width = held.shape[2]
    for d in range(held.shape[0]):
        partial[:, pl.ds(d * width, width)] = jnp.dot(panel, held[d], preferred_element_type=f32).astype(partial.dtype)


def first_body(probes, labels, variances, genotypes, held, partial, panel, current, tags, scales, labels_in, numbers, sems, small, *, snps):
    moves = copies(genotypes, held, sems, True)
    inputs = (
        pltpu.make_async_copy(probes, current, small.at[0]),
        pltpu.make_async_copy(labels, labels_in, small.at[1]),
        pltpu.make_async_copy(variances, numbers, small.at[2]),
    )
    for move in inputs:
        move.start()
    for move in moves:
        move.start()
    for move in inputs:
        move.wait()
    tag = jnp.broadcast_to(labels_in[...], tags.shape)
    tags[...] = tag
    built = build_panel(current[...].astype(f32), tag)
    panel[...] = built
    shape = scales.shape[1:]
    scales[0] = jnp.full(shape, numbers[0] * (1.0 / snps), f32)
    scales[1] = jnp.full(shape, numbers[1] * (1.0 / snps), f32)
    scales[2] = jnp.full(shape, numbers[2], f32)
    for d, move in enumerate(moves):
        move.wait()
        store_bounded(partial, d, jnp.dot(built, held[d], preferred_element_type=f32))


def load_first(probes, labels, variances, genotypes, chips, width, snps):
    count, samples = probes.shape
    rows = ENVS * count
    return pl.pallas_call(
        functools.partial(first_body, snps=snps),
        in_specs=[HBM] * 4,
        out_specs=(VMEM,) * 6,
        out_shape=(
            pltpu.VMEM((chips, samples, width), genotypes.dtype),
            pltpu.VMEM((rows + SCALE_ROWS, chips * width), f32),
            pltpu.VMEM((rows, samples), jnp.bfloat16),
            pltpu.VMEM(probes.shape, probes.dtype),
            pltpu.VMEM(probes.shape, jnp.int32),
            pltpu.VMEM((3,) + probes.shape, f32),
        ),
        scratch_shapes=[
            pltpu.VMEM(labels.shape, labels.dtype),
            pltpu.SMEM(variances.shape, variances.dtype),
            pltpu.SemaphoreType.DMA((chips,)),
            pltpu.SemaphoreType.DMA((3,)),
        ],
        compiler_params=PARAMS,
        name="load_other",
    )(probes, labels, variances, genotypes)


def second_body(panel, genotypes, held, partial, sems):
    moves = copies(genotypes, held, sems, False)
    for move in moves:
        move.start()
    for d, move in enumerate(moves):
        move.wait()
        store_bounded(partial, d, jnp.dot(panel[...], held[d], preferred_element_type=f32))


def load_second(panel, genotypes, chips, width):
    rows, samples = panel.shape
    return pl.pallas_call(
        second_body,
        in_specs=[VMEM, HBM],
        out_specs=(VMEM, VMEM),
        out_shape=(
            pltpu.VMEM((chips, samples, width), genotypes.dtype),
            pltpu.VMEM((rows + SCALE_ROWS, chips * width), f32),
        ),
        scratch_shapes=[pltpu.SemaphoreType.DMA((chips,))],
        compiler_params=PARAMS,
        name="load_own",
    )(panel, genotypes)


def tree_sum(parts):
    while len(parts) > 1:
        parts = [parts[k] + parts[k + 1] for k in range(0, len(parts), 2)]
    return parts[0]


def step_body(current, tags, scales, held, *refs, count):
    first, noise, panel, partial = refs[count:]
    value = tree_sum([refs[k][...] for k in range(count)]) + scales[2] * current[...].astype(f32)
    first[...] = value
    noise[...] = scales[2] * value
    built = build_panel(value.astype(jnp.bfloat16).astype(f32), tags[...])
    panel[...] = built
    products(built, held, partial)


def step_half(current, tags, scales, held, parts, wire):
    rows = ENVS * current.shape[0]
    chips, samples, width = held.shape
    return pl.pallas_call(
        functools.partial(step_body, count=len(parts)),
        in_specs=[VMEM] * (4 + len(parts)),
        out_specs=(VMEM,) * 4,
        out_shape=(
            pltpu.VMEM(current.shape, f32),
            pltpu.VMEM(current.shape, f32),
            pltpu.VMEM((rows, samples), jnp.bfloat16),
            pltpu.VMEM((rows, chips * width), wire),
        ),
        compiler_params=PARAMS,
        name="step_other",
    )(current, tags, scales, held, *parts)


def panel_body(panel, held, partial):
    products(panel[...], held, partial)


def panel_half(panel, held):
    chips, _, width = held.shape
    return pl.pallas_call(
        panel_body,
        in_specs=[VMEM, VMEM],
        out_specs=VMEM,
        out_shape=pltpu.VMEM((panel.shape[0], chips * width), f32),
        compiler_params=PARAMS,
        name="step_own",
    )(panel, held)


def image_body(*refs, blocks, pieces, more, probes):
    panels, refs = refs[:pieces], refs[pieces:]
    held, refs = refs[0], refs[1:]
    width = held.shape[2]
    total = None
    if more:
        total, refs = refs[0][...], refs[1:]
    for k, d in enumerate(blocks):
        per = panels[0].shape[1] // width
        part = panels[k // per][:, pl.ds((k % per) * width, width)]
        term = dot_t(part, held[d])
        total = term if total is None else total + term
    if probes is None:
        refs[0][...] = total
        return
    tags, scales, weighted = refs
    exact = total.shape[0] > ENVS * probes
    tag, additive, interaction = tags[...], scales[0], scales[1]
    skip = probes if exact else 0
    low = jnp.zeros_like(additive) if exact else additive
    high = interaction if exact else additive + interaction
    result = additive * total[:probes] if exact else None
    for e in range(ENVS):
        term = jnp.where(tag == e, high, low) * total[skip + e * probes : skip + (e + 1) * probes]
        result = term if result is None else result + term
    weighted[...] = result


def image(panels, held, blocks, before=None, finish=None):
    rows, samples = panels[0].shape[0], held.shape[1]
    operands = list(panels) + [held] + ([before] if before is not None else [])
    probes = None
    out = pltpu.VMEM((rows, samples), f32)
    if finish is not None:
        operands += list(finish)
        probes = finish[0].shape[0]
        out = pltpu.VMEM(finish[0].shape, f32)
    return pl.pallas_call(
        functools.partial(image_body, blocks=tuple(blocks), pieces=len(panels), more=before is not None, probes=probes),
        in_specs=[VMEM] * len(operands),
        out_specs=VMEM,
        out_shape=out,
        compiler_params=PARAMS,
        name="image",
    )(*operands)


def make(mesh):
    samp, snp = mesh.shape["samp"], mesh.shape["snp"]
    chips = samp // 2
    far = sorted(range(1, chips), key=lambda step: -bin(step).count("1"))
    early = far[: chips // 2 - 1]
    late = far[chips // 2 - 1 :]

    def exchange(block, offset):
        return lax.ppermute(block, "samp", [(k, k ^ offset) for k in range(samp)])

    def between(block, step):
        return exchange(block, 2 * step + step % 2)

    def pack(pair):
        rows, columns = pair.shape[0] - SCALE_ROWS, pair.shape[1]
        exponent = jnp.ceil(jnp.log2(jnp.maximum(pair[rows:], 1e-30)))
        scaled = pair[:rows].reshape(-1, SCALE_ROWS, columns) * jnp.exp2(15.0 - exponent)
        return jnp.concatenate([scaled.reshape(rows, columns), exponent], axis=0).astype(jnp.float16)

    def unpack(block):
        rows, columns = block.shape[0] - SCALE_ROWS, block.shape[1]
        block = block.astype(f32)
        scaled = block[:rows].reshape(-1, SCALE_ROWS, columns) * jnp.exp2(block[rows:] - 15.0)
        return scaled.reshape(rows, columns)

    def reduce_panel(given, own, probes, exact):
        width = own.shape[1] // chips
        rows = ENVS * probes
        pair = own + exchange(given, 1).astype(f32)
        sent = pack(pair) if exact else pair.astype(jnp.bfloat16)
        total = pair[:rows, :width]
        for step in far:
            taken = between(sent[:, step * width : (step + 1) * width], step)
            total = total + (unpack(taken) if exact else taken.astype(f32))
        if exact:
            total = jnp.concatenate([total.reshape(ENVS, probes, width).sum(0), total], axis=0)
        return total.astype(jnp.bfloat16)

    def spread_image(mine, held_own, held_other, finish):
        pieces = {}
        for step in far:
            pieces[step] = between(mine, step)
        other = exchange(mine, 1)
        total = image([mine], held_own, [0])
        total = image([other], held_other, [0], total)
        for step in early:
            other = exchange(pieces[step], 1)
            total = image([pieces[step]], held_own, [step], total)
            total = image([other], held_other, [step], total)
        late_pieces = [pieces[step] for step in late]
        other = exchange(jnp.concatenate(late_pieces, axis=1), 1)
        total = image(late_pieces, held_own, late, total)
        return image([other], held_other, late, total, finish)

    def per_device(genotypes, probes, env_label, variances):
        snps = genotypes.shape[1] * snp
        count = probes.shape[0]
        width = genotypes.shape[1] // samp
        inputs = (genotypes, probes, env_label[None, :], variances)
        genotypes, probes, labels, variances = (pltpu.with_memory_space_constraint(a, pltpu.HBM) for a in inputs)

        def spread(weighted):
            pieces = {
                step: lax.ppermute(weighted, "snp", [(k, k ^ step) for k in range(snp)])
                for step in range(snp - 1, 0, -1)
            }
            return [weighted] + [pieces[step] for step in range(1, snp)]

        held_other, given, panel, current, tags, scales = load_first(probes, labels, variances, genotypes, chips, width, snps)
        held_own, own = load_second(panel, genotypes, chips, width)
        mine = reduce_panel(given, own, count, True)
        parts = spread(spread_image(mine, held_own, held_other, (tags, scales)))
        first, noise, panel, given = step_half(current, tags, scales, held_other, parts, jnp.bfloat16)
        own = panel_half(panel, held_own)
        mine = reduce_panel(given, own, count, False)
        parts = spread(spread_image(mine, held_own, held_other, (tags, scales)))
        return (first, tree_sum(parts) + noise)

    return per_device


def solution(mesh):
    return jax.shard_map(
        make(mesh),
        mesh=mesh,
        in_specs=(P("samp", "snp"), P(None, "samp"), P("samp"), P()),
        out_specs=(P(None, "samp"), P(None, "samp")),
        check_vma=False,
    )
```

```python
import functools

import jax
import jax.numpy as jnp
from jax import lax
from jax.experimental import pallas as pl
from jax.experimental.pallas import tpu as pltpu
from jax.sharding import PartitionSpec as P


ENVS = 8
SCALE_ROWS = 8
VMEM = pl.BlockSpec(memory_space=pltpu.VMEM)
HBM = pl.BlockSpec(memory_space=pltpu.HBM)
PARAMS = pltpu.CompilerParams(vmem_limit_bytes=24 * 1024 * 1024)
f32 = jnp.float32


def build_panel(rounded, tags):
    rows = [jnp.where(tags == e, rounded, 0.0) for e in range(ENVS)]
    return jnp.concatenate(rows, axis=0).astype(jnp.bfloat16)


def dot_t(a, b):
    return lax.dot_general(a, b, (((1,), (1,)), ((), ())), preferred_element_type=f32)


def copies(genotypes, held, sems, other):
    chips, _, width = held.shape
    index = lax.axis_index("samp")
    core, chip = index & 1, index >> 1
    half = core ^ (chip & 1)
    if other:
        half = 1 - half

    def copy(d):
        start = pl.multiple_of((half * chips + (chip ^ d)) * width, width)
        return pltpu.make_async_copy(genotypes.at[:, pl.ds(start, width)], held.at[d], sems.at[d])

    return [copy(d) for d in range(chips)]


def store_bounded(partial, d, block):
    rows, width = block.shape
    partial[pl.ds(0, rows), pl.ds(d * width, width)] = block
    top = jnp.max(jnp.abs(block), axis=0, keepdims=True)
    partial[pl.ds(rows, SCALE_ROWS), pl.ds(d * width, width)] = jnp.broadcast_to(top, (SCALE_ROWS, width))


def products(panel, held, partial):
    width = held.shape[2]
    for d in range(held.shape[0]):
        partial[:, pl.ds(d * width, width)] = jnp.dot(panel, held[d], preferred_element_type=f32).astype(partial.dtype)


def first_body(probes, labels, variances, genotypes, held, partial, panel, current, tags, scales, labels_in, numbers, sems, small, *, snps):
    moves = copies(genotypes, held, sems, True)
    inputs = (
        pltpu.make_async_copy(probes, current, small.at[0]),
        pltpu.make_async_copy(labels, labels_in, small.at[1]),
        pltpu.make_async_copy(variances, numbers, small.at[2]),
    )
    for move in inputs:
        move.start()
    for move in moves:
        move.start()
    for move in inputs:
        move.wait()
    tag = jnp.broadcast_to(labels_in[...], tags.shape)
    tags[...] = tag
    built = build_panel(current[...].astype(f32), tag)
    panel[...] = built
    shape = scales.shape[1:]
    scales[0] = jnp.full(shape, numbers[0] * (1.0 / snps), f32)
    scales[1] = jnp.full(shape, numbers[1] * (1.0 / snps), f32)
    scales[2] = jnp.full(shape, numbers[2], f32)
    for d, move in enumerate(moves):
        move.wait()
        store_bounded(partial, d, jnp.dot(built, held[d], preferred_element_type=f32))


def load_first(probes, labels, variances, genotypes, chips, width, snps):
    count, samples = probes.shape
    rows = ENVS * count
    return pl.pallas_call(
        functools.partial(first_body, snps=snps),
        in_specs=[HBM] * 4,
        out_specs=(VMEM,) * 6,
        out_shape=(
            pltpu.VMEM((chips, samples, width), genotypes.dtype),
            pltpu.VMEM((rows + SCALE_ROWS, chips * width), f32),
            pltpu.VMEM((rows, samples), jnp.bfloat16),
            pltpu.VMEM(probes.shape, probes.dtype),
            pltpu.VMEM(probes.shape, jnp.int32),
            pltpu.VMEM((3,) + probes.shape, f32),
        ),
        scratch_shapes=[
            pltpu.VMEM(labels.shape, labels.dtype),
            pltpu.SMEM(variances.shape, variances.dtype),
            pltpu.SemaphoreType.DMA((chips,)),
            pltpu.SemaphoreType.DMA((3,)),
        ],
        compiler_params=PARAMS,
        name="load_other",
    )(probes, labels, variances, genotypes)


def second_body(panel, genotypes, held, partial, sems):
    moves = copies(genotypes, held, sems, False)
    for move in moves:
        move.start()
    for d, move in enumerate(moves):
        move.wait()
        store_bounded(partial, d, jnp.dot(panel[...], held[d], preferred_element_type=f32))


def load_second(panel, genotypes, chips, width):
    rows, samples = panel.shape
    return pl.pallas_call(
        second_body,
        in_specs=[VMEM, HBM],
        out_specs=(VMEM, VMEM),
        out_shape=(
            pltpu.VMEM((chips, samples, width), genotypes.dtype),
            pltpu.VMEM((rows + SCALE_ROWS, chips * width), f32),
        ),
        scratch_shapes=[pltpu.SemaphoreType.DMA((chips,))],
        compiler_params=PARAMS,
        name="load_own",
    )(panel, genotypes)


def tree_sum(parts):
    while len(parts) > 1:
        parts = [parts[k] + parts[k + 1] for k in range(0, len(parts), 2)]
    return parts[0]


def step_body(current, tags, scales, held, *refs, count):
    first, noise, panel, partial = refs[count:]
    value = tree_sum([refs[k][...] for k in range(count)]) + scales[2] * current[...].astype(f32)
    first[...] = value
    noise[...] = scales[2] * value
    built = build_panel(value.astype(jnp.bfloat16).astype(f32), tags[...])
    panel[...] = built
    products(built, held, partial)


def step_half(current, tags, scales, held, parts, wire):
    rows = ENVS * current.shape[0]
    chips, samples, width = held.shape
    return pl.pallas_call(
        functools.partial(step_body, count=len(parts)),
        in_specs=[VMEM] * (4 + len(parts)),
        out_specs=(VMEM,) * 4,
        out_shape=(
            pltpu.VMEM(current.shape, f32),
            pltpu.VMEM(current.shape, f32),
            pltpu.VMEM((rows, samples), jnp.bfloat16),
            pltpu.VMEM((rows, chips * width), wire),
        ),
        compiler_params=PARAMS,
        name="step_other",
    )(current, tags, scales, held, *parts)


def panel_body(panel, held, partial):
    products(panel[...], held, partial)


def panel_half(panel, held):
    chips, _, width = held.shape
    return pl.pallas_call(
        panel_body,
        in_specs=[VMEM, VMEM],
        out_specs=VMEM,
        out_shape=pltpu.VMEM((panel.shape[0], chips * width), f32),
        compiler_params=PARAMS,
        name="step_own",
    )(panel, held)


def image_body(*refs, blocks, pieces, more, probes):
    panels, refs = refs[:pieces], refs[pieces:]
    held, refs = refs[0], refs[1:]
    width = held.shape[2]
    total = None
    if more:
        total, refs = refs[0][...], refs[1:]
    for k, d in enumerate(blocks):
        per = panels[0].shape[1] // width
        part = panels[k // per][:, pl.ds((k % per) * width, width)]
        term = dot_t(part, held[d])
        total = term if total is None else total + term
    if probes is None:
        refs[0][...] = total
        return
    tags, scales, weighted = refs
    exact = total.shape[0] > ENVS * probes
    tag, additive, interaction = tags[...], scales[0], scales[1]
    skip = probes if exact else 0
    low = jnp.zeros_like(additive) if exact else additive
    high = interaction if exact else additive + interaction
    result = additive * total[:probes] if exact else None
    for e in range(ENVS):
        term = jnp.where(tag == e, high, low) * total[skip + e * probes : skip + (e + 1) * probes]
        result = term if result is None else result + term
    weighted[...] = result


def image(panels, held, blocks, before=None, finish=None):
    rows, samples = panels[0].shape[0], held.shape[1]
    operands = list(panels) + [held] + ([before] if before is not None else [])
    probes = None
    out = pltpu.VMEM((rows, samples), f32)
    if finish is not None:
        operands += list(finish)
        probes = finish[0].shape[0]
        out = pltpu.VMEM(finish[0].shape, f32)
    return pl.pallas_call(
        functools.partial(image_body, blocks=tuple(blocks), pieces=len(panels), more=before is not None, probes=probes),
        in_specs=[VMEM] * len(operands),
        out_specs=VMEM,
        out_shape=out,
        compiler_params=PARAMS,
        name="image",
    )(*operands)


def make(mesh):
    samp, snp = mesh.shape["samp"], mesh.shape["snp"]
    chips = samp // 2
    far = sorted(range(1, chips), key=lambda step: -bin(step).count("1"))
    near = [1] + [step for step in far if step != 1]
    early = near[: chips // 2 - 1]
    late = near[chips // 2 - 1 :]

    def exchange(block, offset):
        return lax.ppermute(block, "samp", [(k, k ^ offset) for k in range(samp)])

    def between(block, step):
        return exchange(block, 2 * step + step % 2)

    def pack(pair):
        rows, columns = pair.shape[0] - SCALE_ROWS, pair.shape[1]
        exponent = jnp.ceil(jnp.log2(jnp.maximum(pair[rows:], 1e-30)))
        scaled = pair[:rows].reshape(-1, SCALE_ROWS, columns) * jnp.exp2(15.0 - exponent)
        return jnp.concatenate([scaled.reshape(rows, columns), exponent], axis=0).astype(jnp.float16)

    def unpack(block):
        rows, columns = block.shape[0] - SCALE_ROWS, block.shape[1]
        block = block.astype(f32)
        scaled = block[:rows].reshape(-1, SCALE_ROWS, columns) * jnp.exp2(block[rows:] - 15.0)
        return scaled.reshape(rows, columns)

    def reduce_panel(given, own, probes, exact):
        width = own.shape[1] // chips
        rows = ENVS * probes
        pair = own + exchange(given, 1).astype(f32)
        sent = pack(pair) if exact else pair.astype(jnp.bfloat16)
        total = pair[:rows, :width]
        for step in far:
            taken = between(sent[:, step * width : (step + 1) * width], step)
            total = total + (unpack(taken) if exact else taken.astype(f32))
        if exact:
            total = jnp.concatenate([total.reshape(ENVS, probes, width).sum(0), total], axis=0)
        return total.astype(jnp.bfloat16)

    def spread_image(mine, held_own, held_other, finish):
        pieces = {}
        for step in near:
            pieces[step] = between(mine, step)
        other = exchange(mine, 1)
        total = image([mine], held_own, [0])
        total = image([other], held_other, [0], total)
        for step in early:
            other = exchange(pieces[step], 1)
            total = image([pieces[step]], held_own, [step], total)
            total = image([other], held_other, [step], total)
        late_pieces = [pieces[step] for step in late]
        other = exchange(jnp.concatenate(late_pieces, axis=1), 1)
        total = image(late_pieces, held_own, late, total)
        return image([other], held_other, late, total, finish)

    def per_device(genotypes, probes, env_label, variances):
        snps = genotypes.shape[1] * snp
        count = probes.shape[0]
        width = genotypes.shape[1] // samp
        inputs = (genotypes, probes, env_label[None, :], variances)
        genotypes, probes, labels, variances = (pltpu.with_memory_space_constraint(a, pltpu.HBM) for a in inputs)

        def spread(weighted):
            pieces = {
                step: lax.ppermute(weighted, "snp", [(k, k ^ step) for k in range(snp)])
                for step in range(snp - 1, 0, -1)
            }
            return [weighted] + [pieces[step] for step in range(1, snp)]

        held_other, given, panel, current, tags, scales = load_first(probes, labels, variances, genotypes, chips, width, snps)
        held_own, own = load_second(panel, genotypes, chips, width)
        mine = reduce_panel(given, own, count, True)
        parts = spread(spread_image(mine, held_own, held_other, (tags, scales)))
        first, noise, panel, given = step_half(current, tags, scales, held_other, parts, jnp.bfloat16)
        own = panel_half(panel, held_own)
        mine = reduce_panel(given, own, count, False)
        parts = spread(spread_image(mine, held_own, held_other, (tags, scales)))
        return (first, tree_sum(parts) + noise)

    return per_device


def solution(mesh):
    return jax.shard_map(
        make(mesh),
        mesh=mesh,
        in_specs=(P("samp", "snp"), P(None, "samp"), P("samp"), P()),
        out_specs=(P(None, "samp"), P(None, "samp")),
        check_vma=False,
    )
```

```python
import functools

import jax
import jax.numpy as jnp
from jax import lax
from jax.experimental import pallas as pl
from jax.experimental.pallas import tpu as pltpu
from jax.sharding import PartitionSpec as P


ENVS = 8
SCALE_ROWS = 8
BEGUN = 1
VMEM = pl.BlockSpec(memory_space=pltpu.VMEM)
HBM = pl.BlockSpec(memory_space=pltpu.HBM)
PARAMS = pltpu.CompilerParams(vmem_limit_bytes=24 * 1024 * 1024)
f32 = jnp.float32


def build_panel(rounded, tags):
    rows = [jnp.where(tags == e, rounded, 0.0) for e in range(ENVS)]
    return jnp.concatenate(rows, axis=0).astype(jnp.bfloat16)


def dot_t(a, b):
    return lax.dot_general(a, b, (((1,), (1,)), ((), ())), preferred_element_type=f32)


def copies(genotypes, held, sems, other, blocks, base=0):
    chips, _, width = held.shape
    index = lax.axis_index("samp")
    core, chip = index & 1, index >> 1
    half = core ^ (chip & 1)
    if other:
        half = 1 - half

    def copy(d):
        start = pl.multiple_of((half * chips + (chip ^ d)) * width, width)
        return pltpu.make_async_copy(genotypes.at[:, pl.ds(start, width)], held.at[d], sems.at[base + d])

    return [copy(d) for d in blocks]


def store_bounded(partial, d, block):
    rows, width = block.shape
    partial[pl.ds(0, rows), pl.ds(d * width, width)] = block
    top = jnp.max(jnp.abs(block), axis=0, keepdims=True)
    partial[pl.ds(rows, SCALE_ROWS), pl.ds(d * width, width)] = jnp.broadcast_to(top, (SCALE_ROWS, width))


def products(panel, held, partial):
    width = held.shape[2]
    for d in range(held.shape[0]):
        partial[:, pl.ds(d * width, width)] = jnp.dot(panel, held[d], preferred_element_type=f32).astype(partial.dtype)


def first_body(
    probes, labels, variances, genotypes,
    held, held_own, partial, panel, current, tags, scales,
    labels_in, numbers, sems, small, *, snps
):
    moves = copies(genotypes, held, sems, True, range(held.shape[0]))
    begun = copies(genotypes, held_own, sems, False, range(BEGUN), held.shape[0])
    inputs = (
        pltpu.make_async_copy(probes, current, small.at[0]),
        pltpu.make_async_copy(labels, labels_in, small.at[1]),
        pltpu.make_async_copy(variances, numbers, small.at[2]),
    )
    for move in inputs:
        move.start()
    for move in moves:
        move.start()
    for move in begun:
        move.start()
    for move in inputs:
        move.wait()
    tag = jnp.broadcast_to(labels_in[...], tags.shape)
    tags[...] = tag
    built = build_panel(current[...].astype(f32), tag)
    panel[...] = built
    shape = scales.shape[1:]
    scales[0] = jnp.full(shape, numbers[0] * (1.0 / snps), f32)
    scales[1] = jnp.full(shape, numbers[1] * (1.0 / snps), f32)
    scales[2] = jnp.full(shape, numbers[2], f32)
    for d, move in enumerate(moves):
        move.wait()
        store_bounded(partial, d, jnp.dot(built, held[d], preferred_element_type=f32))
    for move in begun:
        move.wait()


def load_first(probes, labels, variances, genotypes, chips, width, snps):
    count, samples = probes.shape
    rows = ENVS * count
    return pl.pallas_call(
        functools.partial(first_body, snps=snps),
        in_specs=[HBM] * 4,
        out_specs=(VMEM,) * 7,
        out_shape=(
            pltpu.VMEM((chips, samples, width), genotypes.dtype),
            pltpu.VMEM((chips, samples, width), genotypes.dtype),
            pltpu.VMEM((rows + SCALE_ROWS, chips * width), f32),
            pltpu.VMEM((rows, samples), jnp.bfloat16),
            pltpu.VMEM(probes.shape, probes.dtype),
            pltpu.VMEM(probes.shape, jnp.int32),
            pltpu.VMEM((3,) + probes.shape, f32),
        ),
        scratch_shapes=[
            pltpu.VMEM(labels.shape, labels.dtype),
            pltpu.SMEM(variances.shape, variances.dtype),
            pltpu.SemaphoreType.DMA((chips + BEGUN,)),
            pltpu.SemaphoreType.DMA((3,)),
        ],
        compiler_params=PARAMS,
        name="load_other",
    )(probes, labels, variances, genotypes)


def second_body(panel, genotypes, begun, held, partial, sems):
    chips = held.shape[0]
    moves = copies(genotypes, held, sems, False, range(BEGUN, chips))
    for move in moves:
        move.start()
    for d in range(chips):
        if d >= BEGUN:
            moves[d - BEGUN].wait()
        block = begun[d] if d < BEGUN else held[d]
        store_bounded(partial, d, jnp.dot(panel[...], block, preferred_element_type=f32))


def load_second(panel, genotypes, begun):
    rows = panel.shape[0]
    chips, _, width = begun.shape
    return pl.pallas_call(
        second_body,
        in_specs=[VMEM, HBM, VMEM],
        out_specs=(VMEM, VMEM),
        out_shape=(
            pltpu.VMEM(begun.shape, begun.dtype),
            pltpu.VMEM((rows + SCALE_ROWS, chips * width), f32),
        ),
        input_output_aliases={2: 0},
        scratch_shapes=[pltpu.SemaphoreType.DMA((chips,))],
        compiler_params=PARAMS,
        name="load_own",
    )(panel, genotypes, begun)


def tree_sum(parts):
    while len(parts) > 1:
        parts = [parts[k] + parts[k + 1] for k in range(0, len(parts), 2)]
    return parts[0]


def step_body(current, tags, scales, held, *refs, count):
    first, noise, panel, partial = refs[count:]
    value = tree_sum([refs[k][...] for k in range(count)]) + scales[2] * current[...].astype(f32)
    first[...] = value
    noise[...] = scales[2] * value
    built = build_panel(value.astype(jnp.bfloat16).astype(f32), tags[...])
    panel[...] = built
    products(built, held, partial)


def step_half(current, tags, scales, held, parts, wire):
    rows = ENVS * current.shape[0]
    chips, samples, width = held.shape
    return pl.pallas_call(
        functools.partial(step_body, count=len(parts)),
        in_specs=[VMEM] * (4 + len(parts)),
        out_specs=(VMEM,) * 4,
        out_shape=(
            pltpu.VMEM(current.shape, f32),
            pltpu.VMEM(current.shape, f32),
            pltpu.VMEM((rows, samples), jnp.bfloat16),
            pltpu.VMEM((rows, chips * width), wire),
        ),
        compiler_params=PARAMS,
        name="step_other",
    )(current, tags, scales, held, *parts)


def panel_body(panel, held, partial):
    products(panel[...], held, partial)


def panel_half(panel, held):
    chips, _, width = held.shape
    return pl.pallas_call(
        panel_body,
        in_specs=[VMEM, VMEM],
        out_specs=VMEM,
        out_shape=pltpu.VMEM((panel.shape[0], chips * width), f32),
        compiler_params=PARAMS,
        name="step_own",
    )(panel, held)


def image_body(*refs, blocks, pieces, more, probes):
    panels, refs = refs[:pieces], refs[pieces:]
    held, refs = refs[0], refs[1:]
    width = held.shape[2]
    total = None
    if more:
        total, refs = refs[0][...], refs[1:]
    for k, d in enumerate(blocks):
        per = panels[0].shape[1] // width
        part = panels[k // per][:, pl.ds((k % per) * width, width)]
        term = dot_t(part, held[d])
        total = term if total is None else total + term
    if probes is None:
        refs[0][...] = total
        return
    tags, scales, weighted = refs
    exact = total.shape[0] > ENVS * probes
    tag, additive, interaction = tags[...], scales[0], scales[1]
    skip = probes if exact else 0
    low = jnp.zeros_like(additive) if exact else additive
    high = interaction if exact else additive + interaction
    result = additive * total[:probes] if exact else None
    for e in range(ENVS):
        term = jnp.where(tag == e, high, low) * total[skip + e * probes : skip + (e + 1) * probes]
        result = term if result is None else result + term
    weighted[...] = result


def image(panels, held, blocks, before=None, finish=None):
    rows, samples = panels[0].shape[0], held.shape[1]
    operands = list(panels) + [held] + ([before] if before is not None else [])
    probes = None
    out = pltpu.VMEM((rows, samples), f32)
    if finish is not None:
        operands += list(finish)
        probes = finish[0].shape[0]
        out = pltpu.VMEM(finish[0].shape, f32)
    return pl.pallas_call(
        functools.partial(image_body, blocks=tuple(blocks), pieces=len(panels), more=before is not None, probes=probes),
        in_specs=[VMEM] * len(operands),
        out_specs=VMEM,
        out_shape=out,
        compiler_params=PARAMS,
        name="image",
    )(*operands)


def make(mesh):
    samp, snp = mesh.shape["samp"], mesh.shape["snp"]
    chips = samp // 2
    far = sorted(range(1, chips), key=lambda step: -bin(step).count("1"))
    near = [1] + [step for step in far if step != 1]
    early = near[: chips // 2 - 1]
    late = near[chips // 2 - 1 :]

    def exchange(block, offset):
        return lax.ppermute(block, "samp", [(k, k ^ offset) for k in range(samp)])

    def between(block, step):
        return exchange(block, 2 * step + step % 2)

    def pack(pair):
        rows, columns = pair.shape[0] - SCALE_ROWS, pair.shape[1]
        exponent = jnp.ceil(jnp.log2(jnp.maximum(pair[rows:], 1e-30)))
        scaled = pair[:rows].reshape(-1, SCALE_ROWS, columns) * jnp.exp2(15.0 - exponent)
        return jnp.concatenate([scaled.reshape(rows, columns), exponent], axis=0).astype(jnp.float16)

    def unpack(block):
        rows, columns = block.shape[0] - SCALE_ROWS, block.shape[1]
        block = block.astype(f32)
        scaled = block[:rows].reshape(-1, SCALE_ROWS, columns) * jnp.exp2(block[rows:] - 15.0)
        return scaled.reshape(rows, columns)

    def reduce_panel(given, own, probes, exact):
        width = own.shape[1] // chips
        rows = ENVS * probes
        pair = own + exchange(given, 1).astype(f32)
        sent = pack(pair) if exact else pair.astype(jnp.bfloat16)
        total = pair[:rows, :width]
        for step in far:
            taken = between(sent[:, step * width : (step + 1) * width], step)
            total = total + (unpack(taken) if exact else taken.astype(f32))
        if exact:
            total = jnp.concatenate([total.reshape(ENVS, probes, width).sum(0), total], axis=0)
        return total.astype(jnp.bfloat16)

    def spread_image(mine, held_own, held_other, finish):
        pieces = {}
        for step in near:
            pieces[step] = between(mine, step)
        other = exchange(mine, 1)
        total = image([mine], held_own, [0])
        total = image([other], held_other, [0], total)
        for step in early:
            other = exchange(pieces[step], 1)
            total = image([pieces[step]], held_own, [step], total)
            total = image([other], held_other, [step], total)
        late_pieces = [pieces[step] for step in late]
        other = exchange(jnp.concatenate(late_pieces, axis=1), 1)
        total = image(late_pieces, held_own, late, total)
        return image([other], held_other, late, total, finish)

    def per_device(genotypes, probes, env_label, variances):
        snps = genotypes.shape[1] * snp
        count = probes.shape[0]
        width = genotypes.shape[1] // samp
        inputs = (genotypes, probes, env_label[None, :], variances)
        genotypes, probes, labels, variances = (pltpu.with_memory_space_constraint(a, pltpu.HBM) for a in inputs)

        def spread(weighted):
            pieces = {
                step: lax.ppermute(weighted, "snp", [(k, k ^ step) for k in range(snp)])
                for step in range(snp - 1, 0, -1)
            }
            return [weighted] + [pieces[step] for step in range(1, snp)]

        held_other, begun, given, panel, current, tags, scales = load_first(
            probes, labels, variances, genotypes, chips, width, snps
        )
        held_own, own = load_second(panel, genotypes, begun)
        mine = reduce_panel(given, own, count, True)
        parts = spread(spread_image(mine, held_own, held_other, (tags, scales)))
        first, noise, panel, given = step_half(current, tags, scales, held_other, parts, jnp.bfloat16)
        own = panel_half(panel, held_own)
        mine = reduce_panel(given, own, count, False)
        parts = spread(spread_image(mine, held_own, held_other, (tags, scales)))
        return (first, tree_sum(parts) + noise)

    return per_device


def solution(mesh):
    return jax.shard_map(
        make(mesh),
        mesh=mesh,
        in_specs=(P("samp", "snp"), P(None, "samp"), P("samp"), P()),
        out_specs=(P(None, "samp"), P(None, "samp")),
        check_vma=False,
    )
```

```python
import functools

import jax
import jax.numpy as jnp
from jax import lax
from jax.experimental import pallas as pl
from jax.experimental.pallas import tpu as pltpu
from jax.sharding import PartitionSpec as P


ENVS = 8
SCALE_ROWS = 8
BEGUN = 1
VMEM = pl.BlockSpec(memory_space=pltpu.VMEM)
HBM = pl.BlockSpec(memory_space=pltpu.HBM)
PARAMS = pltpu.CompilerParams(vmem_limit_bytes=24 * 1024 * 1024)
f32 = jnp.float32


def build_panel(rounded, tags):
    rows = [jnp.where(tags == e, rounded, 0.0) for e in range(ENVS)]
    return jnp.concatenate(rows, axis=0).astype(jnp.bfloat16)


def dot_t(a, b):
    return lax.dot_general(a, b, (((1,), (1,)), ((), ())), preferred_element_type=f32)


def copies(genotypes, held, sems, other, blocks, base=0):
    chips, _, width = held.shape
    index = lax.axis_index("samp")
    core, chip = index & 1, index >> 1
    half = core ^ (chip & 1)
    if other:
        half = 1 - half

    def copy(d):
        start = pl.multiple_of((half * chips + (chip ^ d)) * width, width)
        return pltpu.make_async_copy(genotypes.at[:, pl.ds(start, width)], held.at[d], sems.at[base + d])

    return [copy(d) for d in blocks]


def store_bounded(partial, d, block):
    rows, width = block.shape
    partial[pl.ds(0, rows), pl.ds(d * width, width)] = block
    top = jnp.max(jnp.abs(block), axis=0, keepdims=True)
    partial[pl.ds(rows, SCALE_ROWS), pl.ds(d * width, width)] = jnp.broadcast_to(top, (SCALE_ROWS, width))


def products(panel, held, partial):
    width = held.shape[2]
    for d in range(held.shape[0]):
        partial[:, pl.ds(d * width, width)] = jnp.dot(panel, held[d], preferred_element_type=f32).astype(partial.dtype)


def first_body(
    probes, labels, variances, genotypes,
    held, held_own, partial, panel, current, tags, scales,
    labels_in, numbers, sems, small, *, snps
):
    moves = copies(genotypes, held, sems, True, range(held.shape[0]))
    begun = copies(genotypes, held_own, sems, False, range(BEGUN), held.shape[0])
    inputs = (
        pltpu.make_async_copy(probes, current, small.at[0]),
        pltpu.make_async_copy(labels, labels_in, small.at[1]),
        pltpu.make_async_copy(variances, numbers, small.at[2]),
    )
    for move in inputs:
        move.start()
    for move in moves:
        move.start()
    for move in begun:
        move.start()
    for move in inputs:
        move.wait()
    tag = jnp.broadcast_to(labels_in[...], tags.shape)
    tags[...] = tag
    built = build_panel(current[...].astype(f32), tag)
    panel[...] = built
    shape = scales.shape[1:]
    scales[0] = jnp.full(shape, numbers[0] * (1.0 / snps), f32)
    scales[1] = jnp.full(shape, numbers[1] * (1.0 / snps), f32)
    scales[2] = jnp.full(shape, numbers[2], f32)
    for d, move in enumerate(moves):
        move.wait()
        store_bounded(partial, d, jnp.dot(built, held[d], preferred_element_type=f32))
    for move in begun:
        move.wait()


def load_first(probes, labels, variances, genotypes, chips, width, snps):
    count, samples = probes.shape
    rows = ENVS * count
    return pl.pallas_call(
        functools.partial(first_body, snps=snps),
        in_specs=[HBM] * 4,
        out_specs=(VMEM,) * 7,
        out_shape=(
            pltpu.VMEM((chips, samples, width), genotypes.dtype),
            pltpu.VMEM((chips, samples, width), genotypes.dtype),
            pltpu.VMEM((rows + SCALE_ROWS, chips * width), f32),
            pltpu.VMEM((rows, samples), jnp.bfloat16),
            pltpu.VMEM(probes.shape, probes.dtype),
            pltpu.VMEM(probes.shape, jnp.int32),
            pltpu.VMEM((3,) + probes.shape, f32),
        ),
        scratch_shapes=[
            pltpu.VMEM(labels.shape, labels.dtype),
            pltpu.SMEM(variances.shape, variances.dtype),
            pltpu.SemaphoreType.DMA((chips + BEGUN,)),
            pltpu.SemaphoreType.DMA((3,)),
        ],
        compiler_params=PARAMS,
        name="load_other",
    )(probes, labels, variances, genotypes)


def second_body(panel, genotypes, begun, held, partial, sems):
    chips = held.shape[0]
    moves = copies(genotypes, held, sems, False, range(BEGUN, chips))
    for move in moves:
        move.start()
    for d in range(chips):
        if d >= BEGUN:
            moves[d - BEGUN].wait()
        block = begun[d] if d < BEGUN else held[d]
        store_bounded(partial, d, jnp.dot(panel[...], block, preferred_element_type=f32))


def load_second(panel, genotypes, begun):
    rows = panel.shape[0]
    chips, _, width = begun.shape
    return pl.pallas_call(
        second_body,
        in_specs=[VMEM, HBM, VMEM],
        out_specs=(VMEM, VMEM),
        out_shape=(
            pltpu.VMEM(begun.shape, begun.dtype),
            pltpu.VMEM((rows + SCALE_ROWS, chips * width), f32),
        ),
        input_output_aliases={2: 0},
        scratch_shapes=[pltpu.SemaphoreType.DMA((chips,))],
        compiler_params=PARAMS,
        name="load_own",
    )(panel, genotypes, begun)


def tree_sum(parts):
    while len(parts) > 1:
        parts = [parts[k] + parts[k + 1] for k in range(0, len(parts), 2)]
    return parts[0]


def step_body(current, tags, scales, held, *refs, count):
    first, noise, panel, partial = refs[count:]
    value = tree_sum([refs[k][...] for k in range(count)]) + scales[2] * current[...].astype(f32)
    first[...] = value
    noise[...] = scales[2] * value
    built = build_panel(value.astype(jnp.bfloat16).astype(f32), tags[...])
    panel[...] = built
    products(built, held, partial)


def step_half(current, tags, scales, held, parts, wire):
    rows = ENVS * current.shape[0]
    chips, samples, width = held.shape
    return pl.pallas_call(
        functools.partial(step_body, count=len(parts)),
        in_specs=[VMEM] * (4 + len(parts)),
        out_specs=(VMEM,) * 4,
        out_shape=(
            pltpu.VMEM(current.shape, f32),
            pltpu.VMEM(current.shape, f32),
            pltpu.VMEM((rows, samples), jnp.bfloat16),
            pltpu.VMEM((rows, chips * width), wire),
        ),
        compiler_params=PARAMS,
        name="step_other",
    )(current, tags, scales, held, *parts)


def panel_body(panel, held, partial):
    products(panel[...], held, partial)


def panel_half(panel, held):
    chips, _, width = held.shape
    return pl.pallas_call(
        panel_body,
        in_specs=[VMEM, VMEM],
        out_specs=VMEM,
        out_shape=pltpu.VMEM((panel.shape[0], chips * width), f32),
        compiler_params=PARAMS,
        name="step_own",
    )(panel, held)


def image_body(*refs, blocks, pieces, more, probes):
    panels, refs = refs[:pieces], refs[pieces:]
    held, refs = refs[0], refs[1:]
    width = held.shape[2]
    total = None
    if more:
        total, refs = refs[0][...], refs[1:]
    for k, d in enumerate(blocks):
        per = panels[0].shape[1] // width
        part = panels[k // per][:, pl.ds((k % per) * width, width)]
        term = dot_t(part, held[d])
        total = term if total is None else total + term
    if probes is None:
        refs[0][...] = total
        return
    tags, scales, weighted = refs
    exact = total.shape[0] > ENVS * probes
    tag, additive, interaction = tags[...], scales[0], scales[1]
    skip = probes if exact else 0
    low = jnp.zeros_like(additive) if exact else additive
    high = interaction if exact else additive + interaction
    result = additive * total[:probes] if exact else None
    for e in range(ENVS):
        term = jnp.where(tag == e, high, low) * total[skip + e * probes : skip + (e + 1) * probes]
        result = term if result is None else result + term
    weighted[...] = result


def image(panels, held, blocks, before=None, finish=None):
    rows, samples = panels[0].shape[0], held.shape[1]
    operands = list(panels) + [held] + ([before] if before is not None else [])
    probes = None
    out = pltpu.VMEM((rows, samples), f32)
    if finish is not None:
        operands += list(finish)
        probes = finish[0].shape[0]
        out = pltpu.VMEM(finish[0].shape, f32)
    return pl.pallas_call(
        functools.partial(image_body, blocks=tuple(blocks), pieces=len(panels), more=before is not None, probes=probes),
        in_specs=[VMEM] * len(operands),
        out_specs=VMEM,
        out_shape=out,
        compiler_params=PARAMS,
        name="image",
    )(*operands)


def make(mesh):
    samp, snp = mesh.shape["samp"], mesh.shape["snp"]
    chips = samp // 2
    far = sorted(range(1, chips), key=lambda step: -bin(step).count("1"))
    far_down = sorted(far, key=lambda step: (-bin(step).count("1"), -step))
    near = [1] + [step for step in far if step != 1]
    early = near[: chips // 2 - 1]
    late = near[chips // 2 - 1 :]

    def exchange(block, offset):
        return lax.ppermute(block, "samp", [(k, k ^ offset) for k in range(samp)])

    def between(block, step):
        return exchange(block, 2 * step + step % 2)

    def pack(pair):
        rows, columns = pair.shape[0] - SCALE_ROWS, pair.shape[1]
        exponent = jnp.ceil(jnp.log2(jnp.maximum(pair[rows:], 1e-30)))
        scaled = pair[:rows].reshape(-1, SCALE_ROWS, columns) * jnp.exp2(15.0 - exponent)
        return jnp.concatenate([scaled.reshape(rows, columns), exponent], axis=0).astype(jnp.float16)

    def unpack(block):
        rows, columns = block.shape[0] - SCALE_ROWS, block.shape[1]
        block = block.astype(f32)
        scaled = block[:rows].reshape(-1, SCALE_ROWS, columns) * jnp.exp2(block[rows:] - 15.0)
        return scaled.reshape(rows, columns)

    def reduce_panel(given, own, probes, exact):
        order = far if exact else far_down
        width = own.shape[1] // chips
        rows = ENVS * probes
        pair = own + exchange(given, 1).astype(f32)
        sent = pack(pair) if exact else pair.astype(jnp.bfloat16)
        total = pair[:rows, :width]
        for step in order:
            taken = between(sent[:, step * width : (step + 1) * width], step)
            total = total + (unpack(taken) if exact else taken.astype(f32))
        if exact:
            total = jnp.concatenate([total.reshape(ENVS, probes, width).sum(0), total], axis=0)
        return total.astype(jnp.bfloat16)

    def spread_image(mine, held_own, held_other, finish):
        pieces = {}
        for step in near:
            pieces[step] = between(mine, step)
        other = exchange(mine, 1)
        total = image([mine], held_own, [0])
        mine_other = other
        for step in early:
            other = exchange(pieces[step], 1)
            total = image([pieces[step]], held_own, [step], total)
            if step == early[-1]:
                total = image([mine_other, other], held_other, [0, step], total)
            else:
                total = image([other], held_other, [step], total)
        late_pieces = [pieces[step] for step in late]
        other = exchange(jnp.concatenate(late_pieces, axis=1), 1)
        total = image(late_pieces, held_own, late, total)
        return image([other], held_other, late, total, finish)

    def per_device(genotypes, probes, env_label, variances):
        snps = genotypes.shape[1] * snp
        count = probes.shape[0]
        width = genotypes.shape[1] // samp
        inputs = (genotypes, probes, env_label[None, :], variances)
        genotypes, probes, labels, variances = (pltpu.with_memory_space_constraint(a, pltpu.HBM) for a in inputs)

        def spread(weighted):
            pieces = {
                step: lax.ppermute(weighted, "snp", [(k, k ^ step) for k in range(snp)])
                for step in range(1, snp)
            }
            return [weighted] + [pieces[step] for step in range(1, snp)]

        held_other, begun, given, panel, current, tags, scales = load_first(
            probes, labels, variances, genotypes, chips, width, snps
        )
        held_own, own = load_second(panel, genotypes, begun)
        mine = reduce_panel(given, own, count, True)
        parts = spread(spread_image(mine, held_own, held_other, (tags, scales)))
        first, noise, panel, given = step_half(current, tags, scales, held_other, parts, jnp.bfloat16)
        own = panel_half(panel, held_own)
        mine = reduce_panel(given, own, count, False)
        parts = spread(spread_image(mine, held_own, held_other, (tags, scales)))
        return (first, tree_sum(parts) + noise)

    return per_device


def solution(mesh):
    return jax.shard_map(
        make(mesh),
        mesh=mesh,
        in_specs=(P("samp", "snp"), P(None, "samp"), P("samp"), P()),
        out_specs=(P(None, "samp"), P(None, "samp")),
        check_vma=False,
    )
```
